1024 devices in a mesh: dp: 16 (over y_hi, x, core), mp: 64 (over y_lo, z).
Axes of the slice: x: 4, y: 4 (y_hi: 2, y_lo: 2; y = y_hi * 2 + y_lo), z: 32, core: 2. Of those that a mesh axis runs over, the one named last changes fastest.
Arguments:
- tokens: bfloat16 [12288, 6144], P('dp'), may hold values from -60 to 60
- ln_gain: float32 [6144], replicated, may hold values from 0.1 to 1.9
- w_qkv: bfloat16 [6144, 3, 6144], P('dp', None, 'mp'), may hold values from -1 to 1
- q_gain: float32 [128], replicated, may hold values from 0.7 to 2
- k_gain: float32 [128], replicated, may hold values from 0.7 to 2
Outputs:
- context: bfloat16 [12288, 6144], P('dp', 'mp')
The draws below stay inside these ranges and needn't reach their ends.
All inputs are finite; a program needn't handle non-finite values.
Results may differ from the reference program's by a relative error of at most 0.012.
The reference program's roundings to bfloat16 on the way count: a program that leaves them out, or rounds other values in their place, can miss the bound.
Values may be sent and summed in bfloat16 or wider, within the bound.
A program may use at most 64 MiB of HBM per device.

```python
import jax
import jax.numpy as jnp
from jax import lax

D = 6144
HEADS = 48
HEAD_DIM = 128
PATCHES = 256
SPLITS = 4
IMAGES = 48
TOKENS = 12288


def draw_tokens(key, part):
    subkeys = jax.random.split(key, 3)
    row_scale = jnp.exp(jax.random.uniform(subkeys[0], (TOKENS, 1), jnp.float32, -1.2, 1.2))
    col_scale = jnp.exp(jax.random.uniform(subkeys[1], (1, D), jnp.float32, -1.2, 1.2))
    base_draw = jnp.clip(jax.random.normal(subkeys[2], (TOKENS, D), jnp.float32), -4.0, 4.0)
    values = base_draw * row_scale * col_scale
    return jnp.clip(values, -60.0, 60.0).astype(jnp.bfloat16)


def draw_w_qkv(key, part):
    subkeys = jax.random.split(key, 2)
    col_scale = jnp.exp(jax.random.uniform(subkeys[0], (1, 3, D), jnp.float32, -1.0, 1.2))
    base_draw = jnp.clip(jax.random.normal(subkeys[1], (D, 3, D), jnp.float32), -4.0, 4.0)
    values = base_draw * col_scale * D ** (-0.5)
    return jnp.clip(values, -1.0, 1.0).astype(jnp.bfloat16)


def setup_inputs(seed: int = 0) -> dict:
    key_of = jax.random.split(jax.random.key(seed), 6)
    tokens = draw_tokens(jax.random.fold_in(key_of[5], 71), 0)
    ln_gain = jnp.clip(1.0 + 0.18 * jax.random.normal(key_of[1], (D,), jnp.float32), 0.1, 1.9)
    w_qkv = draw_w_qkv(jax.random.fold_in(key_of[5], 71), 0)
    q_gain = jnp.clip(jax.random.uniform(key_of[3], (HEAD_DIM,), jnp.float32, 0.7, 2.0), 0.7, 2.0)
    k_gain = jnp.clip(jax.random.uniform(key_of[4], (HEAD_DIM,), jnp.float32, 0.7, 2.0), 0.7, 2.0)
    return {"tokens": tokens, "ln_gain": ln_gain, "w_qkv": w_qkv, "q_gain": q_gain, "k_gain": k_gain}


norm_eps = 1e-06

def layer_norm(values, gain_vector):
    centre = lax.optimization_barrier(jnp.mean(values, axis=-1, keepdims=True))
    centred = values - centre
    spread = lax.optimization_barrier(jnp.mean(centred * centred, axis=-1, keepdims=True))
    return centred * lax.rsqrt(spread + norm_eps) * gain_vector

def to_heads(features):
    leading = features.shape[:-1]
    parted = features.reshape(leading + (SPLITS, HEADS, HEAD_DIM // SPLITS))
    swapped = jnp.moveaxis(parted, -3, -2)
    return swapped.reshape(leading + (HEADS, HEAD_DIM))

def from_heads(features):
    leading = features.shape[:-2]
    parted = features.reshape(leading + (HEADS, SPLITS, HEAD_DIM // SPLITS))
    swapped = jnp.moveaxis(parted, -2, -3)
    return swapped.reshape(leading + (D,))

def reference(tokens, ln_gain, w_qkv, q_gain, k_gain):
    normed = layer_norm(tokens.astype(jnp.float32), ln_gain).astype(jnp.bfloat16)
    projected = jnp.dot(normed, w_qkv.reshape(D, 3 * D), preferred_element_type=jnp.float32).astype(jnp.bfloat16)
    projected = projected.reshape(IMAGES, PATCHES, 3, D)

    def attend(one_image):
        per_head = to_heads(one_image)
        queries = (layer_norm(per_head[:, 0].astype(jnp.float32), q_gain) * HEAD_DIM ** (-0.5)).astype(jnp.bfloat16)
        key_vecs = layer_norm(per_head[:, 1].astype(jnp.float32), k_gain).astype(jnp.bfloat16)
        values = per_head[:, 2]
        scores = jnp.einsum('qhe,khe->hqk', queries.astype(jnp.float32), key_vecs.astype(jnp.float32))
        raised = jnp.exp(scores)
        weights = (raised / lax.optimization_barrier(jnp.sum(raised, axis=-1, keepdims=True))).astype(jnp.bfloat16)
        attended = jnp.einsum('hqk,khe->qhe', weights.astype(jnp.float32), values.astype(jnp.float32)).astype(jnp.bfloat16)
        return from_heads(attended)
    context = lax.map(attend, projected)
    return context.reshape(TOKENS, D)
```

```python
import functools

import jax
import jax.numpy as jnp
from jax import lax
from jax.experimental import pallas as pl
from jax.experimental.pallas import tpu as pltpu
from jax.sharding import PartitionSpec as P

HEADS = 48
HEAD_DIM = 128
PATCHES = 256
SPLITS = 4
EPS = 1e-06
MESH = pl.DeviceIdType.MESH
PART = HEAD_DIM // SPLITS
LOCAL_HEADS = 3
IMAGES = 3
ROWS = 768
WIDTH = 6144
DEPTH = 384
LN_ROWS = 16


def place():
    dp = lax.axis_index("dp")
    mp = lax.axis_index("mp")
    c = dp % 2
    x = (dp // 2) % 4
    y = (dp // 8) * 2 + mp // 32
    return y + c * (x - y), x + c * (y - x), c, mp % 32


def device(a, b, c, z):
    x = b + c * (a - b)
    y = a + c * (b - a)
    return ((y // 2) * 8 + x * 2 + c, (y % 2) * 32 + z)


def norm_rows(rows, xn, gain_ref):
    x = xn[rows, :].astype(jnp.float32)
    mean = jnp.sum(x, axis=1, keepdims=True) * (1.0 / WIDTH)
    centred = xn[rows, :].astype(jnp.float32) - mean
    spread = jnp.sum(centred * centred, axis=1, keepdims=True) * (1.0 / WIDTH)
    scale = lax.rsqrt(spread + EPS)
    centred = xn[rows, :].astype(jnp.float32) - mean
    xn[rows, :] = (centred * scale * gain_ref[...]).astype(jnp.bfloat16)


def head_norm(pieces, gain):
    values = pieces.astype(jnp.bfloat16).astype(jnp.float32)
    centred = values - jnp.mean(values, axis=1, keepdims=True)
    spread = jnp.mean(centred * centred, axis=1, keepdims=True)
    return centred * lax.rsqrt(spread + EPS) * gain


def gain_row(gain_ref, upper):
    g = [gain_ref[:, r * PART : (r + 1) * PART] for r in range(SPLITS)]
    pick = lambda one, other: jnp.where(upper == 0, one, other)
    return jnp.concatenate(
        [pick(g[0], g[1]), pick(g[2], g[3]), pick(g[1], g[0]), pick(g[3], g[2])], axis=1
    )


def kernel(
    tok_ref, gain_ref, w_ref, q_gain_ref, k_gain_ref, out_ref,
    xn, own, far, val, acc, vt,
    tok_sem, w_sem, z_send, z_recv, one_send, one_recv, two_send, two_recv,
    sib_send, sib_recv, v_send, v_recv, vs_send, vs_recv,
):
    a, b, c, z = place()
    x = b + c * (a - b)
    y = a + c * (b - a)
    yh, yl = y // 2, y % 2
    upper = z // 16
    z_peer = device(a, b, c, (z + 16) % 32)
    sibling = device(y + (1 - c) * (x - y), x + (1 - c) * (y - x), 1 - c, z)
    b_peers = [device(a, (b + j) % 4, c, z) for j in (1, 2, 3)]
    a_peers = [device((a + j) % 4, b, c, z) for j in (1, 2, 3)]
    v_shift = [(1, 0), (2, 0), (3, 0), (0, 2), (1, 2), (2, 2), (3, 2)]

    def v_peer(i, k):
        px, py = (x + i) % 4, (y + k) % 4
        return ((py // 2) * 8 + px * 2 + c, (py % 2) * 32 + z)

    barrier = pltpu.get_barrier_semaphore()
    peers = [z_peer, sibling] + b_peers + a_peers + [v_peer(i, 2) for i in (1, 2, 3)]
    for peer in peers:
        pl.semaphore_signal(barrier, inc=1, device_id=peer, device_id_type=MESH)

    tok_copies = [
        pltpu.make_async_copy(
            tok_ref.at[pl.ds(i * PATCHES, PATCHES)],
            xn.at[pl.ds(i * PATCHES, PATCHES)],
            tok_sem.at[i],
        )
        for i in range(IMAGES)
    ]
    w_copy = pltpu.make_async_copy(w_ref.at[pl.ds(0, 2)], own.at[c, a, b], w_sem.at[0])
    v_copy = pltpu.make_async_copy(w_ref.at[2], val.at[c, yh, x], w_sem.at[1])
    w_copy.start()
    v_copy.start()
    for copy in tok_copies:
        copy.start()

    def remote(src, dst, send, recv, peer):
        return pltpu.make_async_remote_copy(
            src_ref=src, dst_ref=dst, send_sem=send, recv_sem=recv, device_id=peer,
            device_id_type=MESH,
        )

    def same(ref, send, recv, peer):
        return remote(ref, ref, send, recv, peer)

    z_copies = [
        remote(own.at[c, a, b, :, h], far.at[h, c, a, b], z_send.at[h], z_recv.at[h], z_peer)
        for h in range(LOCAL_HEADS)
    ]

    def first(n, ref):
        return [same(ref, one_send.at[n, j], one_recv.at[n, j], b_peers[j]) for j in range(3)]

    def second(n, ref):
        return [same(ref, two_send.at[n, j], two_recv.at[n, j], a_peers[j]) for j in range(3)]

    own_one = first(3, own.at[c, a, b])
    own_two = second(3, own.at[c, a])
    own_sib = same(own.at[c], sib_send.at[3], sib_recv.at[3], sibling)
    far_one = [first(h, far.at[h, c, a, b]) for h in range(LOCAL_HEADS)]
    far_two = [second(h, far.at[h, c, a]) for h in range(LOCAL_HEADS)]
    far_sib = [
        same(far.at[h, c], sib_send.at[h], sib_recv.at[h], sibling) for h in range(LOCAL_HEADS)
    ]
    v_copies = [
        same(val.at[c, yh, x], v_send.at[n], v_recv.at[n], v_peer(i, k))
        for n, (i, k) in enumerate(v_shift)
    ]
    v_sib = same(val.at[c], vs_send, vs_recv, sibling)

    def start(copies):
        for copy in copies:
            copy.start()

    def arrived(copies):
        for copy in copies:
            copy.wait_recv()

    def left(copies):
        for copy in copies:
            copy.wait_send()

    for i in range(IMAGES):
        tok_copies[i].wait()

        def step(n, _):
            base = pl.multiple_of(i * PATCHES + n * LN_ROWS, LN_ROWS)
            norm_rows(pl.ds(base, LN_ROWS), xn, gain_ref)
            return 0

        lax.fori_loop(0, PATCHES // LN_ROWS, step, 0)

    w_copy.wait()
    v_copy.wait()
    pl.semaphore_wait(barrier, len(peers))
    start(z_copies)
    start(own_one)
    start(v_copies)
    arrived(own_one)
    start(own_two)

    def columns(n):
        return pl.ds(pl.multiple_of(n * 2 * DEPTH, 2 * DEPTH), 2 * DEPTH)

    dims = (((1,), (1,)), ((), ()))

    def project_values():
        acc[...] = jnp.zeros_like(acc)

        def step(n, _):
            rhs = jnp.concatenate([val[0, n // 4, n % 4], val[1, n // 4, n % 4]], axis=2)
            rhs = rhs.reshape(LOCAL_HEADS * PART, 2 * DEPTH)
            rhs = jnp.concatenate([rhs, jnp.zeros((PART, 2 * DEPTH), rhs.dtype)], axis=0)
            acc[:, :HEAD_DIM] += lax.dot_general(
                xn[:, columns(n)], rhs, dims, preferred_element_type=jnp.float32
            )
            return 0

        lax.fori_loop(0, 8, step, 0)
        vt[...] = acc[:, :HEAD_DIM].T.astype(jnp.bfloat16)

    def project_head(h):
        acc[...] = jnp.zeros_like(acc)

        def step(n, _):
            hi, col = n // 4, n % 4
            rows = []
            for t in range(2):
                for low in range(2):
                    rows.append(
                        jnp.concatenate(
                            [own[0, hi * 2 + low, col, t, h], own[1, col, hi * 2 + low, t, h]], axis=1
                        )
                    )
                for low in range(2):
                    rows.append(
                        jnp.concatenate(
                            [far[h, 0, hi * 2 + low, col, t], far[h, 1, col, hi * 2 + low, t]], axis=1
                        )
                    )
            rhs = jnp.concatenate(rows, axis=0)
            acc[...] += lax.dot_general(
                xn[:, columns(n)], rhs, dims, preferred_element_type=jnp.float32
            )
            return 0

        lax.fori_loop(0, 8, step, 0)

    q_gain = gain_row(q_gain_ref, upper)
    k_gain = gain_row(k_gain_ref, upper)

    def attend(h):
        for i in range(IMAGES):
            rows = pl.ds(i * PATCHES, PATCHES)
            qn = (head_norm(acc[rows, :HEAD_DIM], q_gain) * HEAD_DIM ** (-0.5)).astype(jnp.bfloat16)
            kn = head_norm(acc[rows, HEAD_DIM:], k_gain).astype(jnp.bfloat16)
            scores = lax.dot_general(kn, qn, dims, preferred_element_type=jnp.float32)
            raised = jnp.exp(scores)
            weights = (raised / jnp.sum(raised, axis=0, keepdims=True)).astype(jnp.bfloat16)
            out_ref[pl.ds(h * PART, PART), rows] = jnp.dot(
                vt[pl.ds(h * PART, PART), rows], weights, preferred_element_type=jnp.float32
            ).astype(jnp.bfloat16)

    arrived([z_copies[0]])
    start(far_one[0])
    arrived(own_two)
    own_sib.start()
    arrived(far_one[0])
    start(far_two[0])
    arrived(v_copies)
    v_sib.start()
    arrived([z_copies[1]])
    start(far_one[1])
    arrived(far_two[0])
    far_sib[0].start()
    arrived(far_one[1])
    start(far_two[1])
    arrived([v_sib, own_sib])
    project_values()
    arrived([z_copies[2]])
    start(far_one[2])
    arrived(far_two[1])
    far_sib[1].start()
    arrived(far_one[2])
    start(far_two[2])
    arrived([far_sib[0]])
    project_head(0)
    attend(0)
    arrived(far_two[2])
    far_sib[2].start()
    arrived([far_sib[1]])
    project_head(1)
    attend(1)
    arrived([far_sib[2]])
    project_head(2)
    attend(2)
    left(z_copies + own_one + own_two + [own_sib, v_sib] + v_copies + far_sib)
    for h in range(LOCAL_HEADS):
        left(far_one[h] + far_two[h])


def body(tokens, ln_gain, w_qkv, q_gain, k_gain):
    w = jnp.transpose(w_qkv, (1, 2, 0)).reshape(3, LOCAL_HEADS, PART, DEPTH)
    vmem = pl.BlockSpec(memory_space=pltpu.VMEM)
    hbm = pl.BlockSpec(memory_space=pl.ANY)
    dma = pltpu.SemaphoreType.DMA
    context = pl.pallas_call(
        kernel,
        out_shape=jax.ShapeDtypeStruct((LOCAL_HEADS * PART, ROWS), jnp.bfloat16),
        in_specs=[hbm, vmem, hbm, vmem, vmem],
        out_specs=vmem,
        scratch_shapes=[
            pltpu.VMEM((ROWS, WIDTH), jnp.bfloat16),
            pltpu.VMEM((2, 4, 4, 2, LOCAL_HEADS, PART, DEPTH), jnp.bfloat16),
            pltpu.VMEM((LOCAL_HEADS, 2, 4, 4, 2, PART, DEPTH), jnp.bfloat16),
            pltpu.VMEM((2, 2, 4, LOCAL_HEADS, PART, DEPTH), jnp.bfloat16),
            pltpu.VMEM((ROWS, 2 * HEAD_DIM), jnp.float32),
            pltpu.VMEM((HEAD_DIM, ROWS), jnp.bfloat16),
            dma((3,)), dma((2,)), dma((3,)), dma((3,)),
            dma((4, 3)), dma((4, 3)), dma((4, 3)), dma((4, 3)),
            dma((4,)), dma((4,)), dma((7,)), dma((7,)), dma, dma,
        ],
        compiler_params=pltpu.CompilerParams(
            collective_id=0, has_side_effects=True, vmem_limit_bytes=60 * 1024 * 1024
        ),
    )(tokens, ln_gain[None, :], w, q_gain[None, :], k_gain[None, :])
    return context.T


def solution(mesh):
    return jax.shard_map(
        body,
        mesh=mesh,
        in_specs=(P("dp", None), P(), P("dp", None, "mp"), P(), P()),
        out_specs=P("dp", "mp"),
        check_vma=False,
    )
```

```python
import jax
import jax.numpy as jnp
from jax import lax
from jax.experimental import pallas as pl
from jax.experimental.pallas import tpu as pltpu
from jax.sharding import PartitionSpec as P

HEADS = 48
HEAD_DIM = 128
PATCHES = 256
SPLITS = 4
EPS = 1e-06
MESH = pl.DeviceIdType.MESH
PART = HEAD_DIM // SPLITS
HALF = HEAD_DIM // 2
LOCAL_HEADS = 3
IMAGES = 3
ROWS = 768
WIDTH = 6144
DEPTH = 384
LN_ROWS = 16
LN_SLICES = 4
LEG = 4
LEGS = 16 // LEG
COPIES = 128
CONTRACT_LAST = (((1,), (1,)), ((), ()))


def norm_rows(base, xn, gain_ref):
    rows = pl.ds(base, LN_ROWS)
    tiles = [pl.ds(128 * t, 128) for t in range(WIDTH // 128)]

    def load(tile):
        return xn[rows, tile].astype(jnp.float32)

    def row_mean(parts):
        total = (parts[0] + parts[1]) + (parts[2] + parts[3])
        return jnp.sum(total, axis=1, keepdims=True) * (1.0 / WIDTH)

    parts = [load(tile) for tile in tiles[:4]]
    for n, tile in enumerate(tiles[4:]):
        parts[n % 4] = parts[n % 4] + load(tile)
    mean = row_mean(parts)
    parts = [None] * 4
    for n, tile in enumerate(tiles):
        centred = load(tile) - mean
        square = centred * centred
        parts[n % 4] = square if n < 4 else parts[n % 4] + square
    scale = lax.rsqrt(row_mean(parts) + EPS)
    for tile in tiles:
        xn[rows, tile] = ((load(tile) - mean) * scale * gain_ref[:, tile]).astype(jnp.bfloat16)


def head_norm(values, gain):
    centred = values - jnp.mean(values, axis=1, keepdims=True)
    spread = jnp.mean(centred * centred, axis=1, keepdims=True)
    return centred * lax.rsqrt(spread + EPS) * gain


def gain_row(gain_ref, upper):
    g = [gain_ref[:, r * PART : (r + 1) * PART] for r in range(SPLITS)]
    pick = lambda one, other: jnp.where(upper == 0, one, other)
    return jnp.concatenate(
        [pick(g[0], g[1]), pick(g[2], g[3]), pick(g[1], g[0]), pick(g[3], g[2])], axis=1
    )


def kernel(
    tok_ref, gain_ref, w_ref, q_gain_ref, k_gain_ref, out_ref,
    xn, q_own, k_own, v_own, q_far, k_far, hop, acc, near, vt, give, take,
    tok_sem, w_sem, send_sem, recv_sem,
):
    dp = lax.axis_index("dp")
    mp = lax.axis_index("mp")
    c, x, yh = dp % 2, (dp // 2) % 4, dp // 8
    yl, z = mp // 32, mp % 32
    y = yh * 2 + yl
    upper = z // 16
    mine = 2 * yl
    other = 2 - 2 * yl
    pair = pl.ds(yl, 2)
    other_pair = pl.ds(1 - yl, 2)

    def device(px, py, pc, pz):
        return ((py // 2) * 8 + px * 2 + pc, (py % 2) * 32 + pz)

    def shifted(i, k):
        return device((x + i) % 4, (y + k) % 4, c, z)

    z_peers = [device(x, y, c, (z + LEG) % 32), device(x, y, c, (z + 32 - LEG) % 32)]
    sibling = device(x, y, 1 - c, z)
    partner = device(x, 2 * yh + 1 - yl, c, z)
    x_peers = [shifted(j, 0) for j in (1, 2, 3)]
    y_peers = [shifted(0, j) for j in (1, 2, 3)]
    shifts = [(i, k) for k in range(4) for i in range(4) if (i, k) != (0, 0)]

    barrier = pltpu.get_barrier_semaphore()
    peers = z_peers + [sibling] + [shifted(i, k) for i, k in shifts]
    for peer in peers:
        pl.semaphore_signal(barrier, inc=1, device_id=peer, device_id_type=MESH)

    w_copies = [
        pltpu.make_async_copy(w_ref.at[0], q_own.at[:, c, y, x], w_sem.at[0]),
        pltpu.make_async_copy(w_ref.at[1], k_own.at[:, c, y, x], w_sem.at[1]),
        pltpu.make_async_copy(w_ref.at[2], v_own.at[:, c, yl, yh, x], w_sem.at[2]),
    ]
    slice_rows = ROWS // LN_SLICES
    tok_copies = [
        pltpu.make_async_copy(
            tok_ref.at[pl.ds(i * slice_rows, slice_rows)],
            xn.at[pl.ds(i * slice_rows, slice_rows)],
            tok_sem.at[i],
        )
        for i in range(LN_SLICES)
    ]
    for copy in w_copies + tok_copies:
        copy.start()

    made = []

    def remote(src, dst, peer):
        n = len(made)
        made.append(
            pltpu.make_async_remote_copy(
                src_ref=src, dst_ref=dst, send_sem=send_sem.at[n], recv_sem=recv_sem.at[n],
                device_id=peer, device_id_type=MESH,
            )
        )
        return made[-1]

    def same(ref, peer):
        return remote(ref, ref, peer)

    def z_leg(leg, h):
        copies = []
        for way, (own, far) in enumerate(((q_own, q_far), (k_own, k_far))):
            src = own.at[h, c, y, x] if leg == 0 else hop.at[leg - 1, way, h]
            dst = far.at[h, c, y, x] if leg == LEGS - 1 else hop.at[leg, way, h]
            copies.append(remote(src, dst, z_peers[way]))
        return copies

    order = (0, 2, 1)
    z_copies = [{h: z_leg(leg, h) for h in order} for leg in range(LEGS)]
    to_y = [(other, other_pair), (mine, pair), (other, other_pair)]
    own_one = [same(q_own.at[:, c, y, x], peer) for peer in x_peers]
    own_one += [same(k_own.at[to_y[j][1], c, y, x], y_peers[j]) for j in range(3)]
    own_two = [same(q_own.at[to_y[j][1], c, y], y_peers[j]) for j in range(3)]
    own_two += [same(k_own.at[pair, c, :, x], peer) for peer in x_peers]
    own_sib = [same(q_own.at[pair, c], sibling), same(k_own.at[pair, c], sibling)]
    v_copies = [
        same(
            v_own.at[pair, c, yl, yh, x] if k % 2 == 0 else v_own.at[other, c, yl, yh, x],
            shifted(i, k),
        )
        for i, k in shifts
    ]
    v_sib = [same(v_own.at[mine, c], sibling), same(v_own.at[1, c, yl], sibling)]
    alone_one = [same(q_far.at[h, c, y, x], peer) for h in (0, 2) for peer in x_peers]
    alone_one += [same(k_far.at[to_y[j][0], c, y, x], y_peers[j]) for j in range(3)]
    alone_two = [same(q_far.at[to_y[j][0], c, y], y_peers[j]) for j in range(3)]
    alone_two += [same(k_far.at[mine, c, :, x], peer) for peer in x_peers]
    alone_sib = [same(q_far.at[mine, c], sibling), same(k_far.at[mine, c], sibling)]
    both_one = [same(q_far.at[1, c, y, x], peer) for peer in x_peers]
    both_one += [same(k_far.at[1, c, y, x], peer) for peer in y_peers]
    both_two = [same(q_far.at[1, c, y], peer) for peer in y_peers]
    both_two += [same(k_far.at[1, c, :, x], peer) for peer in x_peers]
    both_sib = [same(q_far.at[1, c], sibling), same(k_far.at[1, c], sibling)]
    back = remote(give, take, partner)

    def start(copies):
        for copy in copies:
            copy.start()

    def arrived(copies):
        for copy in copies:
            copy.wait_recv()

    def norm_slice(i):
        tok_copies[i].wait()

        def step(n, _):
            norm_rows(pl.multiple_of(i * slice_rows + n * LN_ROWS, LN_ROWS), xn, gain_ref)
            return 0

        lax.fori_loop(0, slice_rows // LN_ROWS, step, 0)

    def relay(leg):
        for h in order:
            for before, after in zip(z_copies[leg - 1][h], z_copies[leg][h]):
                before.wait_recv()
                after.start()

    def project(width, block):
        acc[:, :width] = jnp.zeros((ROWS, width), jnp.float32)

        def step(n, _):
            columns = pl.ds(pl.multiple_of(n * 2 * DEPTH, 2 * DEPTH), 2 * DEPTH)
            rows = [jnp.concatenate(halves, axis=1) for halves in block(n // 4, n % 4)]
            acc[:, :width] += lax.dot_general(
                xn[:, columns], jnp.concatenate(rows, axis=0), CONTRACT_LAST,
                preferred_element_type=jnp.float32,
            )
            return 0

        lax.fori_loop(0, 8, step, 0)

    def head_rows(queries, keys, h, hi, col):
        return [
            [ref[h, 0, hi * 2 + low, col], ref[h, 1, hi * 2 + low, col]]
            for ref in (queries, keys)
            for low in range(2)
        ]

    def project_near():
        project(
            2 * HEAD_DIM,
            lambda hi, col: head_rows(q_own, k_own, mine, hi, col)
            + head_rows(q_own, k_own, 1, hi, col),
        )
        near[...] = acc[...].astype(jnp.bfloat16)

    def project_values():
        def block(hi, col):
            rows = [[v_own[mine, half, low, hi, col] for half in range(2)] for low in (yl, 1 - yl)]
            rows.append([v_own[1, half, yl, hi, col] for half in range(2)])
            return rows + [[jnp.zeros((PART, DEPTH), jnp.bfloat16)] * 2]

        project(HEAD_DIM, block)
        vt[...] = acc[:, :HEAD_DIM].T.astype(jnp.bfloat16)

    def project_far(h):
        project(HEAD_DIM, lambda hi, col: head_rows(q_far, k_far, h, hi, col))

    q_gain = gain_row(q_gain_ref, upper)
    k_gain = gain_row(k_gain_ref, upper)

    def attend(slot, values):
        for i in range(IMAGES):
            rows = pl.ds(i * PATCHES, PATCHES)
            this = near[rows, pl.ds(slot * HEAD_DIM, HEAD_DIM)].astype(jnp.float32)
            that = acc[rows, :HEAD_DIM].astype(jnp.bfloat16).astype(jnp.float32)
            q = jnp.concatenate([this[:, :HALF], that[:, :HALF]], axis=1)
            k = jnp.concatenate([this[:, HALF:], that[:, HALF:]], axis=1)
            qn = (head_norm(q, q_gain) * HEAD_DIM ** (-0.5)).astype(jnp.bfloat16)
            kn = head_norm(k, k_gain).astype(jnp.bfloat16)
            scores = lax.dot_general(kn, qn, CONTRACT_LAST, preferred_element_type=jnp.float32)
            raised = jnp.exp(scores)
            weights = (raised / jnp.sum(raised, axis=0, keepdims=True)).astype(jnp.bfloat16)
            yield rows, jnp.dot(
                vt[values, rows], weights, preferred_element_type=jnp.float32
            ).astype(jnp.bfloat16)

    mine_rows = pl.ds(pl.multiple_of(mine * PART, PART), PART)
    other_rows = pl.ds(pl.multiple_of(other * PART, PART), PART)

    norm_slice(0)
    for copy in w_copies:
        copy.wait()
    pl.semaphore_wait(barrier, len(peers))
    for h in order:
        start(z_copies[0][h])
    start(own_one)
    norm_slice(1)
    relay(1)
    arrived(own_one)
    start(own_two)
    start(v_copies)
    norm_slice(2)
    relay(2)
    norm_slice(3)
    relay(3)
    arrived(own_two)
    start(own_sib)
    arrived(v_copies)
    start(v_sib)
    arrived(z_copies[-1][0] + z_copies[-1][2])
    start(alone_one)
    arrived(z_copies[-1][1])
    start(both_one)
    arrived(own_sib)
    project_near()
    arrived(alone_one)
    start(alone_two)
    arrived(both_one)
    start(both_two)
    arrived(v_sib)
    project_values()
    arrived(alone_two)
    start(alone_sib)
    arrived(alone_sib)
    project_far(mine)
    arrived(both_two)
    start(both_sib)
    for rows, result in attend(0, pl.ds(0, 2 * PART)):
        out_ref[mine_rows, rows] = result[:PART]
        give[:, rows] = result[PART:]
    arrived(both_sib)
    back.start()
    project_far(1)
    for rows, result in attend(1, pl.ds(2 * PART, PART)):
        out_ref[pl.ds(PART, PART), rows] = result
    back.wait_recv()
    out_ref[other_rows, :] = take[...]
    for copy in made:
        copy.wait_send()


def body(tokens, ln_gain, w_qkv, q_gain, k_gain):
    w = jnp.transpose(w_qkv, (1, 2, 0)).reshape(3, LOCAL_HEADS, PART, DEPTH)
    vmem = pl.BlockSpec(memory_space=pltpu.VMEM)
    hbm = pl.BlockSpec(memory_space=pl.ANY)
    dma = pltpu.SemaphoreType.DMA
    gathered = pltpu.VMEM((LOCAL_HEADS, 2, 4, 4, PART, DEPTH), jnp.bfloat16)
    context = pl.pallas_call(
        kernel,
        out_shape=jax.ShapeDtypeStruct((LOCAL_HEADS * PART, ROWS), jnp.bfloat16),
        in_specs=[hbm, vmem, hbm, vmem, vmem],
        out_specs=vmem,
        scratch_shapes=[
            pltpu.VMEM((ROWS, WIDTH), jnp.bfloat16),
            gathered,
            gathered,
            pltpu.VMEM((LOCAL_HEADS, 2, 2, 2, 4, PART, DEPTH), jnp.bfloat16),
            gathered,
            gathered,
            pltpu.VMEM((LEGS - 1, 2, LOCAL_HEADS, PART, DEPTH), jnp.bfloat16),
            pltpu.VMEM((ROWS, 2 * HEAD_DIM), jnp.float32),
            pltpu.VMEM((ROWS, 2 * HEAD_DIM), jnp.bfloat16),
            pltpu.VMEM((HEAD_DIM, ROWS), jnp.bfloat16),
            pltpu.VMEM((PART, ROWS), jnp.bfloat16),
            pltpu.VMEM((PART, ROWS), jnp.bfloat16),
            dma((LN_SLICES,)),
            dma((3,)),
            dma((COPIES,)),
            dma((COPIES,)),
        ],
        compiler_params=pltpu.CompilerParams(
            collective_id=0, has_side_effects=True, vmem_limit_bytes=60 * 1024 * 1024
        ),
    )(tokens, ln_gain[None, :], w, q_gain[None, :], k_gain[None, :])
    return context.T


def solution(mesh):
    return jax.shard_map(
        body,
        mesh=mesh,
        in_specs=(P("dp", None), P(), P("dp", None, "mp"), P(), P()),
        out_specs=P("dp", "mp"),
        check_vma=False,
    )
```

```python
import jax
import jax.numpy as jnp
from jax import lax
from jax.experimental import pallas as pl
from jax.experimental.pallas import tpu as pltpu
from jax.sharding import PartitionSpec as P

HEADS = 48
HEAD_DIM = 128
PATCHES = 256
SPLITS = 4
EPS = 1e-06
MESH = pl.DeviceIdType.MESH
PART = HEAD_DIM // SPLITS
HALF = HEAD_DIM // 2
LOCAL_HEADS = 3
IMAGES = 3
ROWS = 768
WIDTH = 6144
DEPTH = 384
LN_ROWS = 16
LN_SLICES = 4
LEG = 4
LEGS = 16 // LEG
COPIES = 128
CONTRACT_LAST = (((1,), (1,)), ((), ()))


def norm_rows(base, xn, gain_ref):
    rows = pl.ds(base, LN_ROWS)
    tiles = [pl.ds(128 * t, 128) for t in range(WIDTH // 128)]

    def load(tile):
        return xn[rows, tile].astype(jnp.float32)

    def row_mean(parts):
        total = (parts[0] + parts[1]) + (parts[2] + parts[3])
        return jnp.sum(total, axis=1, keepdims=True) * (1.0 / WIDTH)

    parts = [load(tile) for tile in tiles[:4]]
    for n, tile in enumerate(tiles[4:]):
        parts[n % 4] = parts[n % 4] + load(tile)
    mean = row_mean(parts)
    parts = [None] * 4
    for n, tile in enumerate(tiles):
        centred = load(tile) - mean
        square = centred * centred
        parts[n % 4] = square if n < 4 else parts[n % 4] + square
    scale = lax.rsqrt(row_mean(parts) + EPS)
    for tile in tiles:
        xn[rows, tile] = ((load(tile) - mean) * scale * gain_ref[:, tile]).astype(jnp.bfloat16)


def head_norm(values, gain):
    centred = values - jnp.mean(values, axis=1, keepdims=True)
    spread = jnp.mean(centred * centred, axis=1, keepdims=True)
    return centred * lax.rsqrt(spread + EPS) * gain


def gain_row(gain_ref, upper):
    g = [gain_ref[:, r * PART : (r + 1) * PART] for r in range(SPLITS)]
    pick = lambda one, other: jnp.where(upper == 0, one, other)
    return jnp.concatenate(
        [pick(g[0], g[1]), pick(g[2], g[3]), pick(g[1], g[0]), pick(g[3], g[2])], axis=1
    )


def kernel(
    tok_ref, gain_ref, w_ref, q_gain_ref, k_gain_ref, out_ref,
    xn, q_own, k_own, v_own, q_far, k_far, hop, acc, near, vt, give, take,
    tok_sem, w_sem, send_sem, recv_sem,
):
    dp = lax.axis_index("dp")
    mp = lax.axis_index("mp")
    c, x, yh = dp % 2, (dp // 2) % 4, dp // 8
    yl, z = mp // 32, mp % 32
    y = yh * 2 + yl
    upper = z // 16
    mine = 2 * yl
    other = 2 - 2 * yl
    pair = pl.ds(yl, 2)
    other_pair = pl.ds(1 - yl, 2)

    def device(px, py, pc, pz):
        return ((py // 2) * 8 + px * 2 + pc, (py % 2) * 32 + pz)

    def shifted(i, k):
        return device((x + i) % 4, (y + k) % 4, c, z)

    z_peers = [device(x, y, c, (z + LEG) % 32), device(x, y, c, (z + 32 - LEG) % 32)]
    sibling = device(x, y, 1 - c, z)
    partner = device(x, 2 * yh + 1 - yl, c, z)
    x_peers = [shifted(j, 0) for j in (1, 2, 3)]
    y_peers = [shifted(0, j) for j in (1, 2, 3)]
    shifts = [(i, k) for k in range(4) for i in range(4) if (i, k) != (0, 0)]

    barrier = pltpu.get_barrier_semaphore()
    peers = z_peers + [sibling] + [shifted(i, k) for i, k in shifts]
    for peer in peers:
        pl.semaphore_signal(barrier, inc=1, device_id=peer, device_id_type=MESH)

    w_copies = [
        pltpu.make_async_copy(w_ref.at[0], q_own.at[:, c, y, x], w_sem.at[0]),
        pltpu.make_async_copy(w_ref.at[1], k_own.at[:, c, y, x], w_sem.at[1]),
        pltpu.make_async_copy(w_ref.at[2], v_own.at[:, c, yl, yh, x], w_sem.at[2]),
    ]
    slice_rows = ROWS // LN_SLICES
    tok_copies = [
        pltpu.make_async_copy(
            tok_ref.at[pl.ds(i * slice_rows, slice_rows)],
            xn.at[pl.ds(i * slice_rows, slice_rows)],
            tok_sem.at[i],
        )
        for i in range(LN_SLICES)
    ]
    for copy in w_copies + tok_copies:
        copy.start()

    made = []

    def remote(src, dst, peer):
        n = len(made)
        made.append(
            pltpu.make_async_remote_copy(
                src_ref=src, dst_ref=dst, send_sem=send_sem.at[n], recv_sem=recv_sem.at[n],
                device_id=peer, device_id_type=MESH,
            )
        )
        return made[-1]

    def same(ref, peer):
        return remote(ref, ref, peer)

    def z_leg(leg, h):
        copies = []
        for way, (own, far) in enumerate(((q_own, q_far), (k_own, k_far))):
            src = own.at[h, c, y, x] if leg == 0 else hop.at[leg - 1, way, h]
            dst = far.at[h, c, y, x] if leg == LEGS - 1 else hop.at[leg, way, h]
            copies.append(remote(src, dst, z_peers[way]))
        return copies

    def handed(h):
        return [
            copy
            for j in range(4)
            for copy in (
                same(q_far.at[h, c, (y + 4 - j) % 4], sibling),
                same(k_far.at[h, c, :, (x + 4 - j) % 4], sibling),
            )
        ]

    order = (0, 2, 1)
    z_copies = [{h: z_leg(leg, h) for h in order} for leg in range(LEGS)]
    to_y = [(other, other_pair), (mine, pair), (other, other_pair)]
    own_one = [same(q_own.at[:, c, y, x], peer) for peer in x_peers]
    own_one += [same(k_own.at[to_y[j][1], c, y, x], y_peers[j]) for j in range(3)]
    own_two = [same(q_own.at[to_y[j][1], c, y], y_peers[j]) for j in range(3)]
    own_two += [same(k_own.at[pair, c, :, x], peer) for peer in x_peers]
    own_sib = [same(q_own.at[pair, c], sibling), same(k_own.at[pair, c], sibling)]
    v_copies = [
        same(
            v_own.at[pair, c, yl, yh, x] if k % 2 == 0 else v_own.at[other, c, yl, yh, x],
            shifted(i, k),
        )
        for i, k in shifts
    ]
    v_sib = [same(v_own.at[mine, c], sibling), same(v_own.at[1, c, yl], sibling)]
    alone_one = [same(q_far.at[h, c, y, x], peer) for h in (0, 2) for peer in x_peers]
    alone_one += [same(k_far.at[to_y[j][0], c, y, x], y_peers[j]) for j in range(3)]
    alone_two = [same(q_far.at[to_y[j][0], c, y], y_peers[j]) for j in range(3)]
    alone_two += [same(k_far.at[mine, c, :, x], peer) for peer in x_peers]
    alone_sib = handed(mine)
    both_one = [same(q_far.at[1, c, y, x], peer) for peer in x_peers]
    both_one += [same(k_far.at[1, c, y, x], peer) for peer in y_peers]
    both_two = [same(q_far.at[1, c, y], peer) for peer in y_peers]
    both_two += [same(k_far.at[1, c, :, x], peer) for peer in x_peers]
    both_sib = handed(1)
    back = remote(give, take, partner)

    def start(copies):
        for copy in copies:
            copy.start()

    def arrived(copies):
        for copy in copies:
            copy.wait_recv()

    def hand_over(two, sib):
        for j in range(3):
            arrived([two[j], two[3 + j]])
            start(sib[2 * j + 2 : 2 * j + 4])

    def norm_slice(i):
        tok_copies[i].wait()

        def step(n, _):
            norm_rows(pl.multiple_of(i * slice_rows + n * LN_ROWS, LN_ROWS), xn, gain_ref)
            return 0

        lax.fori_loop(0, slice_rows // LN_ROWS, step, 0)

    def relay(leg):
        for h in order:
            for before, after in zip(z_copies[leg - 1][h], z_copies[leg][h]):
                before.wait_recv()
                after.start()

    def project(width, block):
        acc[:, :width] = jnp.zeros((ROWS, width), jnp.float32)

        def step(n, _):
            columns = pl.ds(pl.multiple_of(n * 4 * DEPTH, 4 * DEPTH), 4 * DEPTH)
            hi, col = n // 2, (n % 2) * 2
            rows = [
                jnp.concatenate(left + right, axis=1)
                for left, right in zip(block(hi, col), block(hi, col + 1))
            ]
            acc[:, :width] += lax.dot_general(
                xn[:, columns], jnp.concatenate(rows, axis=0), CONTRACT_LAST,
                preferred_element_type=jnp.float32,
            )
            return 0

        lax.fori_loop(0, 4, step, 0)

    def head_rows(queries, keys, h, hi, col):
        return [
            [ref[h, 0, hi * 2 + low, col], ref[h, 1, hi * 2 + low, col]]
            for ref in (queries, keys)
            for low in range(2)
        ]

    def project_near():
        project(
            2 * HEAD_DIM,
            lambda hi, col: head_rows(q_own, k_own, mine, hi, col)
            + head_rows(q_own, k_own, 1, hi, col),
        )
        near[...] = acc[...].astype(jnp.bfloat16)

    def project_values():
        def block(hi, col):
            rows = [[v_own[mine, half, low, hi, col] for half in range(2)] for low in (yl, 1 - yl)]
            rows.append([v_own[1, half, yl, hi, col] for half in range(2)])
            return rows + [[jnp.zeros((PART, DEPTH), jnp.bfloat16)] * 2]

        project(HEAD_DIM, block)
        vt[...] = acc[:, :HEAD_DIM].T.astype(jnp.bfloat16)

    def project_far(h):
        project(HEAD_DIM, lambda hi, col: head_rows(q_far, k_far, h, hi, col))

    q_gain = gain_row(q_gain_ref, upper)
    k_gain = gain_row(k_gain_ref, upper)

    def attend(slot, values):
        for i in range(IMAGES):
            rows = pl.ds(i * PATCHES, PATCHES)
            this = near[rows, pl.ds(slot * HEAD_DIM, HEAD_DIM)].astype(jnp.float32)
            that = acc[rows, :HEAD_DIM].astype(jnp.bfloat16).astype(jnp.float32)
            q = jnp.concatenate([this[:, :HALF], that[:, :HALF]], axis=1)
            k = jnp.concatenate([this[:, HALF:], that[:, HALF:]], axis=1)
            qn = (head_norm(q, q_gain) * HEAD_DIM ** (-0.5)).astype(jnp.bfloat16)
            kn = head_norm(k, k_gain).astype(jnp.bfloat16)
            scores = lax.dot_general(kn, qn, CONTRACT_LAST, preferred_element_type=jnp.float32)
            raised = jnp.exp(scores)
            weights = (raised / jnp.sum(raised, axis=0, keepdims=True)).astype(jnp.bfloat16)
            yield rows, jnp.dot(
                vt[values, rows], weights, preferred_element_type=jnp.float32
            ).astype(jnp.bfloat16)

    mine_rows = pl.ds(pl.multiple_of(mine * PART, PART), PART)
    other_rows = pl.ds(pl.multiple_of(other * PART, PART), PART)

    norm_slice(0)
    for copy in w_copies:
        copy.wait()
    pl.semaphore_wait(barrier, len(peers))
    for h in order:
        start(z_copies[0][h])
    start(own_one)
    norm_slice(1)
    relay(1)
    arrived(own_one)
    start(own_two)
    start(v_copies)
    norm_slice(2)
    relay(2)
    norm_slice(3)
    relay(3)
    arrived(own_two)
    start(own_sib)
    arrived(v_copies)
    start(v_sib)
    arrived(z_copies[-1][0] + z_copies[-1][2])
    start(alone_one)
    arrived(z_copies[-1][1])
    start(both_one)
    arrived(own_sib)
    project_near()
    arrived(alone_one)
    start(alone_two + alone_sib[:2])
    arrived(both_one)
    start(both_two + both_sib[:2])
    arrived(v_sib)
    project_values()
    hand_over(alone_two, alone_sib)
    arrived(alone_sib)
    project_far(mine)
    hand_over(both_two, both_sib)
    for rows, result in attend(0, pl.ds(0, 2 * PART)):
        out_ref[mine_rows, rows] = result[:PART]
        give[:, rows] = result[PART:]
    arrived(both_sib)
    back.start()
    project_far(1)
    for rows, result in attend(1, pl.ds(2 * PART, PART)):
        out_ref[pl.ds(PART, PART), rows] = result
    back.wait_recv()
    out_ref[other_rows, :] = take[...]
    for copy in made:
        copy.wait_send()


def body(tokens, ln_gain, w_qkv, q_gain, k_gain):
    w = jnp.transpose(w_qkv, (1, 2, 0)).reshape(3, LOCAL_HEADS, PART, DEPTH)
    vmem = pl.BlockSpec(memory_space=pltpu.VMEM)
    hbm = pl.BlockSpec(memory_space=pl.ANY)
    dma = pltpu.SemaphoreType.DMA
    gathered = pltpu.VMEM((LOCAL_HEADS, 2, 4, 4, PART, DEPTH), jnp.bfloat16)
    context = pl.pallas_call(
        kernel,
        out_shape=jax.ShapeDtypeStruct((LOCAL_HEADS * PART, ROWS), jnp.bfloat16),
        in_specs=[hbm, vmem, hbm, vmem, vmem],
        out_specs=vmem,
        scratch_shapes=[
            pltpu.VMEM((ROWS, WIDTH), jnp.bfloat16),
            gathered,
            gathered,
            pltpu.VMEM((LOCAL_HEADS, 2, 2, 2, 4, PART, DEPTH), jnp.bfloat16),
            gathered,
            gathered,
            pltpu.VMEM((LEGS - 1, 2, LOCAL_HEADS, PART, DEPTH), jnp.bfloat16),
            pltpu.VMEM((ROWS, 2 * HEAD_DIM), jnp.float32),
            pltpu.VMEM((ROWS, 2 * HEAD_DIM), jnp.bfloat16),
            pltpu.VMEM((HEAD_DIM, ROWS), jnp.bfloat16),
            pltpu.VMEM((PART, ROWS), jnp.bfloat16),
            pltpu.VMEM((PART, ROWS), jnp.bfloat16),
            dma((LN_SLICES,)),
            dma((3,)),
            dma((COPIES,)),
            dma((COPIES,)),
        ],
        compiler_params=pltpu.CompilerParams(
            collective_id=0, has_side_effects=True, vmem_limit_bytes=60 * 1024 * 1024
        ),
    )(tokens, ln_gain[None, :], w, q_gain[None, :], k_gain[None, :])
    return context.T


def solution(mesh):
    return jax.shard_map(
        body,
        mesh=mesh,
        in_specs=(P("dp", None), P(), P("dp", None, "mp"), P(), P()),
        out_specs=P("dp", "mp"),
        check_vma=False,
    )
```
